1024 devices in a mesh: grid: 64 (over x, z_lo, core), shard: 16 (over y, z_hi).
Axes of the slice: x: 8, y: 8, z: 8 (z_hi: 2, z_lo: 4; z = z_hi * 4 + z_lo), core: 2. Of those that a mesh axis runs over, the one named last changes fastest.
Arguments:
- density: float32 [64, 256, 16, 512], P('grid', 'shard'), may hold values from -1.6 to 1.6
- coefficients: int32 [64], P('grid'), may hold values from -2 to 2
- offsets: int32 [64, 6], P('grid'), may hold values from 0 to 3
- fractions: float32 [64, 6], P('grid'), may hold values from 0.05 to 0.95
- subspace_ids: int32 [64, 256, 16], P('grid', 'shard'), may hold values from 0 to 1023, as said below
Outputs:
- combined: float32 [64, 256, 16, 512], P('grid', 'shard')
The draws below stay inside these ranges and needn't reach their ends.
Inputs may be any that keep to these rules, and one draw needn't show every extreme that they name: `subspace_ids`: cut each grid's blocks b = i0 * 16 + i1 into runs of 256 consecutive blocks. Within one run at most 8 ids lie in any one range r * 16 to r * 16 + 15, and in every run one such range, the same for all grids at that run, holds exactly 8.
All inputs are finite; a program needn't handle non-finite values.
Results may differ from the reference program's by a relative error of at most 0.0003.
Values sent between devices are 32-bit elements; how exact they have to be, the bound alone decides.
A program may use at most 128 MiB of HBM per device.

```python
import jax
import jax.numpy as jnp
import numpy as np
from jax import lax

CA = 16
M2 = 8
M3 = 4
M4 = 4
M5 = 4
OWN = 16
GROUPS = 64
A = 256
B = 16
TAIL = 512
BLK_DEV = 256
NG = 1024
CAP = 8
N_SHARD = 16


def draw_subspace_ids(key, part):
    run_count = GROUPS * (A // CA)
    slot_count = CAP * GROUPS
    first_key, second_key, third_key, fourth_key = jax.random.split(key, 4)
    favored = jax.random.randint(first_key, (A // CA,), 0, GROUPS)
    favored_run = jnp.tile(favored, GROUPS)
    ranking = jax.vmap(lambda sub_key: jax.random.permutation(sub_key, slot_count))(jax.random.split(second_key, run_count))
    slot_owner = jnp.arange(slot_count, dtype=jnp.int32) // CAP
    scores = ranking.astype(jnp.int32) + slot_count * (slot_owner[None, :] != favored_run[:, None]).astype(jnp.int32)
    ordering = jnp.argsort(scores, axis=1, stable=True)
    chosen = ordering[:, :BLK_DEV].astype(jnp.int32) // CAP
    mixing = jax.vmap(lambda sub_key: jax.random.permutation(sub_key, BLK_DEV))(jax.random.split(third_key, run_count))
    owners = jnp.take_along_axis(chosen, mixing.astype(jnp.int32), axis=1)
    within = jax.random.randint(fourth_key, (run_count, BLK_DEV), 0, OWN)
    return (owners * OWN + within).astype(jnp.int32).reshape(GROUPS, A, B)


def set_ends(array, key, low, largest):
    shape = array.shape
    place = [jax.random.randint(jax.random.fold_in(key, axis), (), 0, shape[axis]) for axis in range(len(shape))]
    array = array.at[tuple(place)].set(low)
    longest = shape.index(max(shape))
    place[longest] = (place[longest] + 1) % shape[longest]
    return array.at[tuple(place)].set(largest)


def levels(own_key, dims, cuts, low, largest):
    def one(dim, parts):
        heights = jax.random.uniform(jax.random.fold_in(jax.random.fold_in(own_key, 6), dim), (parts,), jnp.float32, low / len(cuts), largest / len(cuts))
        return jnp.repeat(jnp.exp(heights), dims[dim] // parts).reshape((-1,) + (1,) * (len(dims) - dim - 1))

    gain = one(*cuts[0])
    for cut in cuts[1:]:
        gain = gain * one(*cut)
    return gain


def bell_draw(rng, dims, width, limit, pieces=(), kind=jnp.bfloat16):
    level = levels(rng, dims, pieces, -0.22, 0.18) if pieces else 1.0
    array = jax.random.normal(rng, dims, jnp.float32) * width * level
    return jnp.minimum(jnp.maximum(array, -limit), limit).astype(kind)


def setup_inputs(seed: int = 0) -> dict:
    streams_of = jax.random.split(jax.random.key(seed), 6)
    return {
        "density": bell_draw(streams_of[0], (GROUPS, A, B, TAIL), 0.2, 1.6, ((0, 64), (1, 16)), jnp.float32),
        "coefficients": set_ends(jax.random.randint(streams_of[1], (GROUPS,), -2, 3), jax.random.fold_in(streams_of[1], 1), -2, 2).astype(jnp.int32),
        "offsets": set_ends(jax.random.randint(streams_of[2], (GROUPS, 6), 0, 4), jax.random.fold_in(streams_of[2], 1), 0, 3).astype(jnp.int32),
        "fractions": jnp.clip(0.05 + 0.9 * jax.random.uniform(streams_of[3], (GROUPS, 6), jnp.float32) ** levels(streams_of[3], (GROUPS, 6), ((0, 64),), -0.2, 0.2), 0.05, 0.95),
        "subspace_ids": draw_subspace_ids(jax.random.fold_in(streams_of[5], 71), 0),
    }


highest = lax.Precision.HIGHEST


def hier_table(length):
    matrix = np.eye(length)
    for level_index in range(length.bit_length() - 1):
        spacing = 2 ** level_index
        for position in range(spacing, length, 2 * spacing):
            matrix[position] = matrix[position] - 0.5 * (matrix[position - spacing] + matrix[(position + spacing) % length])
    return matrix.astype(np.float32)


def dehier_table(length):
    matrix = np.eye(length)
    for level_index in reversed(range(length.bit_length() - 1)):
        spacing = 2 ** level_index
        for position in range(spacing, length, 2 * spacing):
            matrix[position] = matrix[position] + 0.5 * (matrix[position - spacing] + matrix[(position + spacing) % length])
    return matrix.astype(np.float32)


def sweep_matrix(length, shift, fraction):
    row_index = jnp.arange(length, dtype=jnp.int32)[:, None]
    column_index = jnp.arange(length, dtype=jnp.int32)[None, :]
    remain = 1.0 - fraction
    weights = (-remain * (remain - 1.0) * (remain - 2.0) / 6.0,
               (remain + 1.0) * (remain - 1.0) * (remain - 2.0) / 2.0,
               -(remain + 1.0) * remain * (remain - 2.0) / 2.0,
               (remain + 1.0) * remain * (remain - 1.0) / 6.0)
    matrix = jnp.zeros((length, length), jnp.float32)
    for stencil, weight in enumerate(weights):
        source = jnp.mod(row_index - shift - 2 + stencil, length)
        matrix = matrix + jnp.where(source == column_index, weight, 0.0)
    return matrix


def operator_pair(length, shift, fraction):
    return jnp.dot(jnp.asarray(hier_table(length), jnp.float32), sweep_matrix(length, shift, fraction), precision=highest)


def along_axis(volume, matrix, axis_index):
    moved = jnp.tensordot(matrix, volume, axes=([1], [axis_index]), precision=highest)
    return jnp.moveaxis(moved, 0, axis_index)


def reference(density, coefficients, offsets, fractions, subspace_ids):
    shape_six = (A, B, M2, M3, M4, M5)

    def forward(inputs):
        volume, shifts, fraction_row = inputs
        volume = volume.reshape(shape_six)
        for axis_index in range(6):
            volume = along_axis(volume, operator_pair(shape_six[axis_index], shifts[axis_index], fraction_row[axis_index]), axis_index)
        return volume.reshape(A * B, TAIL)

    hierarchized = lax.map(forward, (density, offsets, fractions))
    scaled = hierarchized * coefficients.astype(jnp.float32)[:, None, None]
    block_index = jnp.arange(A * B, dtype=jnp.int32)
    global_ids = (block_index // BLK_DEV * NG)[None, :] + subspace_ids.reshape(GROUPS, A * B).astype(jnp.int32)
    sparse = jax.ops.segment_sum(scaled.reshape(GROUPS * A * B, TAIL), global_ids.reshape(-1), num_segments=N_SHARD * NG)
    returned = jnp.take(sparse, global_ids, axis=0)

    def backward(volume):
        volume = volume.reshape(shape_six)
        for axis_index in range(6):
            volume = along_axis(volume, jnp.asarray(dehier_table(shape_six[axis_index]), jnp.float32), axis_index)
        return volume.reshape(A, B, TAIL)

    return lax.map(backward, returned)
```

```python
import functools

import jax
import jax.numpy as jnp
import numpy as np
from jax import lax
from jax.experimental import pallas as pl
from jax.experimental.pallas import tpu as pltpu
from jax.sharding import PartitionSpec as P

MESH = pl.DeviceIdType.MESH
CORES = 2
GROUP = 32
LANES = 128
TAIL_DIMS = (8, 4, 4, 4)
IDS = 1024

f32 = jnp.float32
bf16 = jnp.bfloat16


def dehier_table(length):
    matrix = np.eye(length)
    for level_index in reversed(range(length.bit_length() - 1)):
        spacing = 2**level_index
        for position in range(spacing, length, 2 * spacing):
            matrix[position] = matrix[position] + 0.5 * (
                matrix[position - spacing] + matrix[(position + spacing) % length]
            )
    return matrix


def iota(shape, dim):
    return lax.broadcasted_iota(jnp.int32, shape, dim)


def split(value):
    high = value.astype(bf16)
    return high, (value - high.astype(f32)).astype(bf16)


def dot(left, right):
    return jnp.dot(left, right, preferred_element_type=f32)


def dot_t(left, right):
    return lax.dot_general(left, right, (((1,), (1,)), ((), ())), preferred_element_type=f32)


def stencil_weights(fraction):
    r = 1.0 - fraction
    sixth = 1.0 / 6.0
    return (
        -r * (r - 1.0) * (r - 2.0) * sixth,
        (r + 1.0) * (r - 1.0) * (r - 2.0) * 0.5,
        -(r + 1.0) * r * (r - 2.0) * 0.5,
        (r + 1.0) * r * (r - 1.0) * sixth,
    )


def sweep(row, col, length, shift, weights):
    step = (col - row + (shift + 2)) & (length - 1)
    out = jnp.where(step == 3, weights[3], 0.0)
    for k in range(3):
        out = jnp.where(step == k, weights[k], out)
    return out


def forward_entry(row, col, length, shift, weights):
    low = row & (-row)
    here = sweep(row, col, length, shift, weights)
    sides = sweep(row - low, col, length, shift, weights) + sweep(
        row + low, col, length, shift, weights
    )
    return jnp.where(row == 0, here, here - 0.5 * sides)


def swap_groups(tiles):
    lane = iota(tiles[0].shape, 1)
    low64 = lane < 64
    even32 = (lane & 32) == 0
    half = [None] * 4
    for a in (0, 1):
        b = a + 2
        half[a] = jnp.where(low64, tiles[a], pltpu.roll(tiles[b], 64, 1))
        half[b] = jnp.where(low64, pltpu.roll(tiles[a], 64, 1), tiles[b])
    done = [None] * 4
    for a in (0, 2):
        b = a + 1
        done[a] = jnp.where(even32, half[a], pltpu.roll(half[b], 32, 1))
        done[b] = jnp.where(even32, pltpu.roll(half[a], 96, 1), half[b])
    return done


def spread_groups(value):
    value = value + pltpu.roll(value, 64, 1)
    return value + pltpu.roll(value, 32, 1)


def step_kernel(
    cfg,
    coef,
    shifts,
    fracs,
    x_ref,
    ids_ref,
    dlead_hbm,
    dsecond_hbm,
    dtail_hbm,
    out_ref,
    dlead,
    dsecond,
    dtail,
    chi,
    clo,
    pxs,
    thi,
    tlo,
    lhi,
    llo,
    vbuf,
    wbuf,
    rbuf,
    fbuf,
    gbuf,
    idown,
    idall,
    idmine,
    idrow,
    hot,
    hot_t,
    rhs,
    acc,
    table,
    zrecv,
    zsum,
    tsum,
    tsplit,
    abuf,
    bbuf,
    obuf,
    ubuf,
    const_sem,
    id_send,
    id_recv,
    send_sem,
    recv_sem,
    z_send,
    z_recv,
):
    S, ZN, AL, BN, NQ = cfg.shards, cfg.zs, cfg.rows, cfg.second, cfg.chunks
    A, TAIL = cfg.lead, cfg.tail
    ROWS = AL * BN
    g = lax.axis_index("grid")
    s = lax.axis_index("shard")
    core = lax.rem(g, CORES)
    zz = lax.rem(g // CORES, ZN)
    xx = g // (CORES * ZN)
    own = xx * CORES + core

    def owner_grid(o):
        return ((o // CORES) * ZN + zz) * CORES + lax.rem(o, CORES)

    def z_grid(z):
        return (xx * ZN + z) * CORES + core

    barrier = pltpu.get_barrier_semaphore()

    def greet(k, carry):
        pl.semaphore_signal(
            barrier, inc=1, device_id=(g, lax.rem(s + k, S)), device_id_type=MESH
        )
        pl.semaphore_signal(
            barrier, inc=1, device_id=(owner_grid(lax.rem(own + k, S)), s), device_id_type=MESH
        )
        return carry

    lax.fori_loop(1, S, greet, 0)

    def greet_z(k, carry):
        pl.semaphore_signal(
            barrier, inc=1, device_id=(z_grid(lax.rem(zz + k, ZN)), s), device_id_type=MESH
        )
        return carry

    lax.fori_loop(1, ZN, greet_z, 0)

    consts = [
        pltpu.make_async_copy(dlead_hbm, dlead, const_sem.at[0]),
        pltpu.make_async_copy(dsecond_hbm, dsecond, const_sem.at[1]),
        pltpu.make_async_copy(dtail_hbm, dtail, const_sem.at[2]),
    ]
    for copy in consts:
        copy.start()

    weights = [stencil_weights(fracs[0, d]) for d in range(6)]
    shift = [shifts[0, d] for d in range(6)]

    idown[...] = jnp.zeros_like(idown)
    idown[:, 0:BN] = ids_ref[...].astype(f32)

    RB = 32

    def build_second(i, carry):
        row = iota((RB, ROWS), 0) + i * RB
        col = iota((RB, ROWS), 1)
        entry = forward_entry(row // AL, col & (BN - 1), BN, shift[1], weights[1])
        entry = jnp.where((row & (AL - 1)) == col // BN, entry, 0.0)
        high, low = split(entry)
        chi[pl.ds(i * RB, RB), :] = high
        clo[pl.ds(i * RB, RB), :] = low
        return carry

    lax.fori_loop(0, ROWS // RB, build_second, 0)

    n2, n3, n4, n5 = cfg.tail_dims
    PN, QN = n2 * n3, n4 * n5
    prow, pcol = iota((PN, TAIL), 0), iota((PN, TAIL), 1) // QN
    first = forward_entry(prow // n3, pcol // n3, n2, shift[2], weights[2])
    if n3 > 1:
        first = first * forward_entry(
            prow & (n3 - 1), pcol & (n3 - 1), n3, shift[3], weights[3]
        )
    pxs[...] = first
    qrow, qcol = iota((QN, TAIL), 0), iota((QN, TAIL), 1) & (QN - 1)
    last = forward_entry(qrow // n5, qcol // n5, n4, shift[4], weights[4]) * forward_entry(
        qrow & (n5 - 1), qcol & (n5 - 1), n5, shift[5], weights[5]
    )

    def build_tail(i, carry):
        high, low = split(pxs[pl.ds(i, 1), :] * last)
        thi[pl.ds(i * QN, QN), :] = high
        tlo[pl.ds(i * QN, QN), :] = low
        return carry

    lax.fori_loop(0, PN, build_tail, 0)

    xh, xl = split(x_ref[...])
    u = dot(chi[...], xh) + dot(chi[...], xl) + dot(clo[...], xh)
    uh, ul = split(u)
    vbuf[...] = dot_t(uh, thi[...]) + dot_t(uh, tlo[...]) + dot_t(ul, thi[...])

    PG = TAIL // LANES
    for q in range(NQ):
        for p in range(PG):
            tiles = [
                vbuf[pl.ds((4 * q + j) * AL, AL), pl.ds(p * LANES, LANES)] for j in range(4)
            ]
            for i, tile in enumerate(swap_groups(tiles)):
                wbuf[q, 4 * p + i] = tile

    pl.semaphore_wait(barrier, 2 * (S - 1) + (ZN - 1))

    def send_ids(k, carry):
        to = lax.rem(s + k, S)
        pltpu.make_async_remote_copy(
            idown,
            idall.at[s],
            id_send.at[0],
            id_recv.at[0],
            device_id=(g, to),
            device_id_type=MESH,
        ).start()
        return carry

    lax.fori_loop(1, S, send_ids, 0)

    def send_to_shards(src, dst_of, phase, q):
        def body(k, carry):
            to = lax.rem(s + k, S)
            pltpu.make_async_remote_copy(
                src(to),
                dst_of,
                send_sem.at[phase, q],
                recv_sem.at[phase, q],
                device_id=(g, to),
                device_id_type=MESH,
            ).start()
            return carry

        lax.fori_loop(1, S, body, 0)

    def send_to_owners(src, dst_of, phase, q):
        def body(k, carry):
            to = lax.rem(own + k, S)
            pltpu.make_async_remote_copy(
                src(to),
                dst_of,
                send_sem.at[phase, q],
                recv_sem.at[phase, q],
                device_id=(owner_grid(to), s),
                device_id_type=MESH,
            ).start()
            return carry

        lax.fori_loop(1, S, body, 0)

    def all_bytes(ref, sem):
        pltpu.make_async_copy(ref, ref, sem).wait()

    peers = pl.ds(0, S - 1)

    for q in range(NQ):
        send_to_shards(lambda to: wbuf.at[q, to], rbuf.at[q, s], 0, q)
        rbuf[q, pl.ds(s, 1)] = wbuf[q, pl.ds(s, 1)]

    scale = coef[0].astype(f32)
    scaled = [w * scale for w in weights[0]]

    def build_lead(i, carry):
        row = iota((RB, A), 0) + i * RB
        col = iota((RB, A), 1)
        high, low = split(forward_entry(row, col, A, shift[0], scaled))
        lhi[pl.ds(i * RB, RB), :] = high
        llo[pl.ds(i * RB, RB), :] = low
        return carry

    lax.fori_loop(0, A // RB, build_lead, 0)

    idall[pl.ds(s, 1)] = idown[...][None]
    all_bytes(idall.at[peers], id_recv.at[0])

    def send_ids_on(k, carry):
        to = lax.rem(own + k, S)
        pltpu.make_async_remote_copy(
            idall.at[to],
            idmine.at[own],
            id_send.at[1],
            id_recv.at[1],
            device_id=(owner_grid(to), s),
            device_id_type=MESH,
        ).start()
        return carry

    lax.fori_loop(1, S, send_ids_on, 0)
    idmine[pl.ds(own, 1)] = idall[pl.ds(own, 1)]

    GA = S * AL
    NG = cfg.ids

    def build_hot(q):
        for j in range(4):
            b = 4 * q + j
            ids_here = idrow[b : b + 1, :]
            column = idmine[...].reshape(GA, LANES)[:, b : b + 1].astype(jnp.int32)

            def rows(i, carry):
                number = iota((RB, GA), 0) + i * RB
                hot[q, pl.ds(i * RB, RB), j * GA : (j + 1) * GA] = jnp.where(
                    number == ids_here, 1.0, 0.0
                ).astype(bf16)
                return carry

            lax.fori_loop(0, NG // RB, rows, 0)
            for i in range(GA // RB):
                hot_t[q, j * GA + i * RB : j * GA + (i + 1) * RB, :] = jnp.where(
                    iota((RB, NG), 1) == column[i * RB : (i + 1) * RB], 1.0, 0.0
                ).astype(bf16)

    lane_group = iota((1, LANES), 1) // GROUP

    for q in range(NQ):
        all_bytes(rbuf.at[q, peers], recv_sem.at[0, q])
        rh, rl = split(rbuf[q].reshape(A, LANES))
        fbuf[q] = (dot(lhi[...], rh) + dot(lhi[...], rl) + dot(llo[...], rh)).reshape(
            S, AL, LANES
        )
        send_to_owners(lambda to: fbuf.at[q, to], gbuf.at[q, own], 1, q)
        gbuf[q, pl.ds(own, 1)] = fbuf[q, pl.ds(own, 1)]
        if q == 0:
            all_bytes(idmine.at[peers], id_recv.at[1])
            idrow[...] = jnp.transpose(idmine[...].reshape(GA, LANES)).astype(jnp.int32)
        build_hot(q)

    acc[...] = jnp.zeros_like(acc)

    for q in range(NQ):
        all_bytes(gbuf.at[q, peers], recv_sem.at[1, q])
        value = gbuf[q].reshape(GA, LANES)
        high = value.astype(bf16).astype(f32)
        low = value - high
        for j in range(4):
            here = lane_group == j
            rhs[j * GA : (j + 1) * GA, 0:LANES] = jnp.where(here, high, 0.0).astype(bf16)
            rhs[j * GA : (j + 1) * GA, LANES:] = jnp.where(here, low, 0.0).astype(bf16)
        acc[...] += dot(hot[q], rhs[...])

    QI = NG // 4
    packed = jnp.zeros((QI, LANES), f32)
    for k in range(4):
        part = acc[k * QI : (k + 1) * QI, :]
        packed = jnp.where(
            lane_group == k, spread_groups(part[:, :LANES] + part[:, LANES:]), packed
        )
    ZR = QI // ZN
    table[...] = packed.reshape(ZN, ZR, LANES)

    def send_z(k, carry):
        to = lax.rem(zz + k, ZN)
        pltpu.make_async_remote_copy(
            table.at[to],
            zrecv.at[zz],
            z_send.at[0],
            z_recv.at[0],
            device_id=(z_grid(to), s),
            device_id_type=MESH,
        ).start()
        return carry

    lax.fori_loop(1, ZN, send_z, 0)
    zrecv[pl.ds(zz, 1)] = table[pl.ds(zz, 1)]
    zpeers = pl.ds(0, ZN - 1)
    all_bytes(zrecv.at[zpeers], z_recv.at[0])
    total = zrecv[0]
    for k in range(1, ZN):
        total = total + zrecv[k]
    zsum[...] = total

    def send_sum(k, carry):
        to = lax.rem(zz + k, ZN)
        pltpu.make_async_remote_copy(
            zsum,
            tsum.at[zz],
            z_send.at[1],
            z_recv.at[1],
            device_id=(z_grid(to), s),
            device_id_type=MESH,
        ).start()
        return carry

    lax.fori_loop(1, ZN, send_sum, 0)
    tsum[pl.ds(zz, 1)] = total[None]
    all_bytes(tsum.at[zpeers], z_recv.at[1])
    packed = tsum[...].reshape(QI, LANES)
    for k in range(4):
        high, low = split(spread_groups(jnp.where(lane_group == k, packed, 0.0)))
        tsplit[k * QI : (k + 1) * QI, 0:LANES] = high
        tsplit[k * QI : (k + 1) * QI, LANES:] = low

    for q in range(NQ):
        answer = jnp.zeros((GA, LANES), f32)
        for j in range(4):
            rows_j = dot(hot_t[q, j * GA : (j + 1) * GA, :], tsplit[...])
            answer = jnp.where(lane_group == j, rows_j[:, :LANES] + rows_j[:, LANES:], answer)
        abuf[q] = answer.reshape(S, AL, LANES)
        send_to_owners(lambda to: abuf.at[q, to], bbuf.at[q, own], 2, q)
        bbuf[q, pl.ds(own, 1)] = abuf[q, pl.ds(own, 1)]

    for copy in consts:
        copy.wait()

    for q in range(NQ):
        all_bytes(bbuf.at[q, peers], recv_sem.at[2, q])
        bh, bl = split(bbuf[q].reshape(A, LANES))
        obuf[q] = (dot(dlead[...], bh) + dot(dlead[...], bl)).reshape(S, AL, LANES)
        send_to_shards(lambda to: obuf.at[q, to], ubuf.at[q, s], 3, q)
        ubuf[q, pl.ds(s, 1)] = obuf[q, pl.ds(s, 1)]

    for q in range(NQ):
        all_bytes(ubuf.at[q, peers], recv_sem.at[3, q])
        for p in range(PG):
            for j, tile in enumerate(swap_groups([ubuf[q, 4 * p + i] for i in range(4)])):
                vbuf[pl.ds((4 * q + j) * AL, AL), pl.ds(p * LANES, LANES)] = tile

    vh, vl = split(vbuf[...])
    y = dot_t(vh, dtail[...]) + dot_t(vl, dtail[...])
    yh, yl = split(y)
    out_ref[...] = dot(dsecond[...], yh) + dot(dsecond[...], yl)

    all_bytes(idall.at[peers], id_send.at[0])
    all_bytes(idall.at[peers], id_send.at[1])
    all_bytes(table.at[zpeers], z_send.at[0])
    all_bytes(tsum.at[zpeers], z_send.at[1])
    for phase in range(4):
        for q in range(NQ):
            all_bytes(wbuf.at[q, peers], send_sem.at[phase, q])


class Config:
    pass


def run_step(cfg, x, coef, shifts, fracs, ids):
    S, ZN, AL, BN, NQ = cfg.shards, cfg.zs, cfg.rows, cfg.second, cfg.chunks
    A, TAIL, NG = cfg.lead, cfg.tail, cfg.ids
    GA, ROWS, QI = S * AL, AL * BN, NG // 4
    n2, n3, n4, n5 = cfg.tail_dims
    dlead = jnp.asarray(dehier_table(A), bf16)
    second = np.einsum("bc,ad->abcd", dehier_table(BN), np.eye(AL)).reshape(ROWS, ROWS)
    dsecond = jnp.asarray(second, bf16)
    dtail = jnp.asarray(
        functools.reduce(np.kron, [dehier_table(n) for n in cfg.tail_dims]), bf16
    )
    vmem, smem = pl.BlockSpec(memory_space=pltpu.VMEM), pl.BlockSpec(memory_space=pltpu.SMEM)
    hbm = pl.BlockSpec(memory_space=pl.ANY)
    V, D = pltpu.VMEM, pltpu.SemaphoreType.DMA
    slabs = V((NQ, S, AL, LANES), f32)
    return pl.pallas_call(
        functools.partial(step_kernel, cfg),
        out_shape=jax.ShapeDtypeStruct((ROWS, TAIL), f32),
        in_specs=[smem, smem, smem, vmem, vmem, hbm, hbm, hbm],
        out_specs=vmem,
        scratch_shapes=[
            V((A, A), bf16),
            V((ROWS, ROWS), bf16),
            V((TAIL, TAIL), bf16),
            V((ROWS, ROWS), bf16),
            V((ROWS, ROWS), bf16),
            V((n2 * n3, TAIL), f32),
            V((TAIL, TAIL), bf16),
            V((TAIL, TAIL), bf16),
            V((A, A), bf16),
            V((A, A), bf16),
            V((ROWS, TAIL), f32),
            slabs,
            slabs,
            slabs,
            slabs,
            V((AL, LANES), f32),
            V((S, AL, LANES), f32),
            V((S, AL, LANES), f32),
            V((LANES, GA), jnp.int32),
            V((NQ, NG, 4 * GA), bf16),
            V((NQ, 4 * GA, NG), bf16),
            V((4 * GA, 2 * LANES), bf16),
            V((NG, 2 * LANES), f32),
            V((ZN, QI // ZN, LANES), f32),
            V((ZN, QI // ZN, LANES), f32),
            V((QI // ZN, LANES), f32),
            V((ZN, QI // ZN, LANES), f32),
            V((NG, 2 * LANES), bf16),
            slabs,
            slabs,
            slabs,
            slabs,
            D((3,)),
            D((2,)),
            D((2,)),
            D((4, NQ)),
            D((4, NQ)),
            D((2,)),
            D((2,)),
        ],
        compiler_params=pltpu.CompilerParams(
            collective_id=0, has_side_effects=True, vmem_limit_bytes=60 * 1024 * 1024
        ),
    )(coef, shifts, fracs, x, ids, dlead, dsecond, dtail)


def build(mesh, tail_dims, id_count):
    def body(density, coefficients, offsets, fractions, subspace_ids):
        _, rows, second, tail = density.shape
        cfg = Config()
        cfg.shards = mesh.shape["shard"]
        cfg.zs = mesh.shape["grid"] // cfg.shards
        cfg.rows, cfg.second, cfg.tail = rows, second, tail
        cfg.lead = rows * cfg.shards
        cfg.chunks = second * GROUP // LANES
        cfg.tail_dims, cfg.ids = tail_dims, id_count
        out = run_step(
            cfg,
            density.reshape(rows * second, tail),
            coefficients,
            offsets,
            fractions,
            subspace_ids[0],
        )
        return out.reshape(density.shape)

    return jax.shard_map(
        body,
        mesh=mesh,
        in_specs=(
            P("grid", "shard", None, None),
            P("grid"),
            P("grid", None),
            P("grid", None),
            P("grid", "shard", None),
        ),
        out_specs=P("grid", "shard", None, None),
        check_vma=False,
    )


def solution(mesh):
    return build(mesh, TAIL_DIMS, IDS)
```

```python
import functools

import jax
import jax.numpy as jnp
from jax import lax
from jax.experimental import pallas as pl
from jax.experimental.pallas import tpu as pltpu
from jax.sharding import PartitionSpec as P

MESH = pl.DeviceIdType.MESH
CORES = 2
GROUP = 32
LANES = 128
TAIL_DIMS = (8, 4, 4, 4)
IDS = 1024
PACK = 8
PARTS = 1

f32 = jnp.float32
bf16 = jnp.bfloat16


def iota(shape, dim):
    return lax.broadcasted_iota(jnp.int32, shape, dim)


def split(value):
    high = value.astype(bf16)
    return high, (value - high.astype(f32)).astype(bf16)


def dot(left, right):
    return jnp.dot(left, right, preferred_element_type=f32)


def dot_t(left, right):
    return lax.dot_general(left, right, (((1,), (1,)), ((), ())), preferred_element_type=f32)


def stencil_weights(fraction):
    r = 1.0 - fraction
    sixth = 1.0 / 6.0
    return (
        -r * (r - 1.0) * (r - 2.0) * sixth,
        (r + 1.0) * (r - 1.0) * (r - 2.0) * 0.5,
        -(r + 1.0) * r * (r - 2.0) * 0.5,
        (r + 1.0) * r * (r - 1.0) * sixth,
    )


def sweep(row, col, length, shift, weights):
    step = (col - row + (shift + 2)) & (length - 1)
    out = jnp.where(step == 3, weights[3], 0.0)
    for k in range(3):
        out = jnp.where(step == k, weights[k], out)
    return out


def forward_entry(row, col, length, shift, weights):
    low = row & (-row)
    here = sweep(row, col, length, shift, weights)
    sides = sweep(row - low, col, length, shift, weights) + sweep(
        row + low, col, length, shift, weights
    )
    return jnp.where(row == 0, here, here - 0.5 * sides)


def backward_entry(row, col):
    width = (col & (-col)).astype(f32)
    away = jnp.abs(row - col).astype(f32)
    hat = jnp.maximum(width - away, 0.0) / jnp.where(col == 0, 1.0, width)
    return jnp.where(col == 0, 1.0, hat)


def swap_groups(tiles):
    lane = iota(tiles[0].shape, 1)
    low64 = lane < 64
    even32 = (lane & 32) == 0
    half = [None] * 4
    for a in (0, 1):
        b = a + 2
        half[a] = jnp.where(low64, tiles[a], pltpu.roll(tiles[b], 64, 1))
        half[b] = jnp.where(low64, pltpu.roll(tiles[a], 64, 1), tiles[b])
    done = [None] * 4
    for a in (0, 2):
        b = a + 1
        done[a] = jnp.where(even32, half[a], pltpu.roll(half[b], 32, 1))
        done[b] = jnp.where(even32, pltpu.roll(half[a], 96, 1), half[b])
    return done


def step_kernel(
    cfg,
    coef_hbm,
    shifts_hbm,
    fracs_hbm,
    x_hbm,
    ids_hbm,
    out_ref,
    coef,
    shifts,
    fracs,
    ids_ref,
    xbuf,
    dlead,
    dsecond,
    dtail,
    chi,
    clo,
    pxs,
    thi,
    tlo,
    lhi,
    llo,
    vbuf,
    wbuf,
    rbuf,
    fbuf,
    gbuf,
    idwide,
    idown,
    idall,
    idmine,
    idcol,
    idrow,
    quarter,
    hot,
    hot_t,
    rhs,
    acc,
    table,
    zrecv,
    zsum,
    tsum,
    tsplit,
    abuf,
    bbuf,
    obuf,
    ubuf,
    x_sem,
    id_send,
    id_recv,
    send_sem,
    recv_sem,
    z_send,
    z_recv,
):
    S, ZN, AL, BN, NQ = cfg.shards, cfg.zs, cfg.rows, cfg.second, cfg.chunks
    A, TAIL = cfg.lead, cfg.tail
    ROWS = AL * BN
    AH, NG = PARTS, cfg.ids
    RA, BQ, QI = AL // AH, 4 // AH, NG // 4
    GR = S * RA
    g = lax.axis_index("grid")
    s = lax.axis_index("shard")
    core = lax.rem(g, CORES)
    zz = lax.rem(g // CORES, ZN)
    xx = g // (CORES * ZN)
    own = xx * CORES + core

    def owner_grid(o):
        return ((o // CORES) * ZN + zz) * CORES + lax.rem(o, CORES)

    def z_grid(z):
        return (xx * ZN + z) * CORES + core

    copies = [
        pltpu.make_async_copy(src, dst, x_sem.at[k])
        for k, (src, dst) in enumerate(
            [
                (ids_hbm, ids_ref),
                (shifts_hbm, shifts),
                (fracs_hbm, fracs),
                (x_hbm, xbuf),
                (coef_hbm, coef),
            ]
        )
    ]
    for copy in copies:
        copy.start()
    barrier = pltpu.get_barrier_semaphore()

    def far_first(me, send):
        ring = S // 2
        u, v = me // 2, lax.rem(me, 2)

        def body(i, carry):
            sign = 1 - 2 * lax.rem(i, 2)
            step = ring // 2 + sign * ((i + 1) // 2)
            to = lax.rem(u + step + ring, ring) * 2
            send(to + 1 - v)
            send(to + v)
            return carry

        lax.fori_loop(0, ring - 1, body, 0)
        send(u * 2 + 1 - v)

    def greet(grid, shard):
        pl.semaphore_signal(barrier, inc=1, device_id=(grid, shard), device_id_type=MESH)

    far_first(s, lambda to: greet(g, to))
    far_first(own, lambda to: greet(owner_grid(to), s))

    def greet_z(k, carry):
        greet(z_grid(lax.rem(zz + k, ZN)), s)
        return carry

    lax.fori_loop(1, ZN, greet_z, 0)
    copies[0].wait()
    copies[1].wait()
    copies[2].wait()
    weights = [stencil_weights(fracs[0, d]) for d in range(6)]
    shift = [shifts[0, d] for d in range(6)]

    idwide[...] = jnp.zeros_like(idwide)
    idwide[:, 0:BN] = ids_ref[...].astype(f32)
    wide = idwide[...]
    for step in (BN, 2 * BN, 4 * BN):
        wide = wide + pltpu.roll(wide, step, 1)
    mine = (iota((AL, LANES), 1) // BN) == (iota((AL, LANES), 0) & (PACK - 1))
    wide = jnp.where(mine, wide, 0.0)
    for k in range(AL // PACK):
        idown[k : k + 1, :] = jnp.sum(
            wide[k * PACK : (k + 1) * PACK], axis=0, keepdims=True
        )

    RB = 32
    cells = forward_entry(
        iota((BN, ROWS), 0), iota((BN, ROWS), 1) & (BN - 1), BN, shift[1], weights[1]
    )
    own_row = iota((AL, ROWS), 0) == iota((AL, ROWS), 1) // BN
    for b in range(BN):
        high, low = split(jnp.where(own_row, cells[b : b + 1], 0.0))
        chi[b * AL : (b + 1) * AL, :] = high
        clo[b * AL : (b + 1) * AL, :] = low

    n2, n3, n4, n5 = cfg.tail_dims
    PN, QN = n2 * n3, n4 * n5
    prow, pcol = iota((PN, TAIL), 0), iota((PN, TAIL), 1) // QN
    first = forward_entry(prow // n3, pcol // n3, n2, shift[2], weights[2])
    if n3 > 1:
        first = first * forward_entry(
            prow & (n3 - 1), pcol & (n3 - 1), n3, shift[3], weights[3]
        )
    pxs[...] = first
    qrow, qcol = iota((QN, TAIL), 0), iota((QN, TAIL), 1) & (QN - 1)
    last = forward_entry(qrow // n5, qcol // n5, n4, shift[4], weights[4]) * forward_entry(
        qrow & (n5 - 1), qcol & (n5 - 1), n5, shift[5], weights[5]
    )

    def build_tail(i, carry):
        high, low = split(pxs[pl.ds(i, 1), :] * last)
        thi[pl.ds(i * QN, QN), :] = high
        tlo[pl.ds(i * QN, QN), :] = low
        return carry

    lax.fori_loop(0, PN, build_tail, 0)

    copies[3].wait()
    copies[4].wait()
    xh, xl = split(xbuf[...])
    u = dot(chi[...], xh) + dot(chi[...], xl) + dot(clo[...], xh)
    uh, ul = split(u)
    vbuf[...] = dot_t(uh, thi[...]) + dot_t(uh, tlo[...]) + dot_t(ul, thi[...])

    pl.semaphore_wait(barrier, 2 * (S - 1) + (ZN - 1))

    def to_shard(src, dst, send_at, recv_at):
        def send(to):
            pltpu.make_async_remote_copy(
                src(to), dst, send_at, recv_at, device_id=(g, to), device_id_type=MESH
            ).start()

        far_first(s, send)

    def to_owner(src, dst, send_at, recv_at):
        def send(to):
            pltpu.make_async_remote_copy(
                src(to),
                dst,
                send_at,
                recv_at,
                device_id=(owner_grid(to), s),
                device_id_type=MESH,
            ).start()

        far_first(own, send)

    to_shard(lambda to: idown, idall.at[s], id_send.at[0], id_recv.at[0])

    def send_to_shards(src, dst, phase, q):
        to_shard(src, dst, send_sem.at[phase, q], recv_sem.at[phase, q])

    def send_to_owners(src, dst, phase, q):
        to_owner(src, dst, send_sem.at[phase, q], recv_sem.at[phase, q])

    def all_bytes(ref, sem):
        pltpu.make_async_copy(ref, ref, sem).wait()

    peers = pl.ds(0, S - 1)

    PG = TAIL // LANES

    def group_row(q, j):
        return (q * BQ + j % BQ) * AL + j // BQ * RA

    for q in range(NQ):
        for p in range(PG):
            tiles = [
                vbuf[pl.ds(group_row(q, j), RA), pl.ds(p * LANES, LANES)] for j in range(4)
            ]
            for i, tile in enumerate(swap_groups(tiles)):
                wbuf[q, 4 * p + i] = tile
        send_to_shards(lambda to: wbuf.at[q, to], rbuf.at[q, s], 0, q)
        rbuf[q, pl.ds(s, 1)] = wbuf[q, pl.ds(s, 1)]

    scale = coef[0].astype(f32)
    scaled = [w * scale for w in weights[0]]

    def lead_row_col(i):
        row, col = iota((RB, GR), 0) + i * RB, iota((RB, GR), 1)
        out, part = row & (A - 1), row // A
        return (
            (out & (GR - 1)) // RA * AL + out // GR * RA + (out & (RA - 1)),
            col // RA * AL + part * RA + (col & (RA - 1)),
        )

    def build_lead(i, carry):
        row, col = lead_row_col(i)
        high, low = split(forward_entry(row, col, A, shift[0], scaled))
        lhi[pl.ds(i * RB, RB), :] = high
        llo[pl.ds(i * RB, RB), :] = low
        return carry

    lax.fori_loop(0, AH * A // RB, build_lead, 0)

    low64 = iota((1, LANES), 1) < 64

    def lead_apply(value, high, low):
        vh, vl = split(value)
        both = dot(high[...], jnp.concatenate([vh, vl], axis=1))
        out = both[:, :LANES] + both[:, LANES:]
        if low is not None:
            out = out + dot(low[...], vh)
        if AH == 1:
            return out.reshape(S, RA, LANES)
        out = jnp.where(low64, out[:A], out[A:])
        out = out + pltpu.roll(out, 64, 1)
        return jnp.where(low64, out[:GR], out[GR:]).reshape(S, RA, LANES)

    idall[pl.ds(s, 1)] = idown[...][None]
    all_bytes(idall.at[peers], id_recv.at[0])

    to_owner(lambda to: idall.at[to], idmine.at[own], id_send.at[1], id_recv.at[1])
    idmine[pl.ds(own, 1)] = idall[pl.ds(own, 1)]

    def build_hot(q):
        for j in range(4):
            at = j // BQ * BN + q * BQ + j % BQ
            ids_here = idrow[at : at + 1, :] & (QI - 1)
            hot[q, :, j * GR : (j + 1) * GR] = jnp.where(
                iota((QI, GR), 0) == ids_here, 1.0, 0.0
            ).astype(bf16)
            column = idcol[:, at : at + 1]
            quarter[q, j] = jnp.broadcast_to(column // QI, (GR, LANES))
            hot_t[q, j * GR : (j + 1) * GR, :] = jnp.where(
                iota((GR, QI), 1) == (column & (QI - 1)), 1.0, 0.0
            ).astype(bf16)

    lane_group = iota((1, LANES), 1) // GROUP

    def lead_step(q):
        all_bytes(rbuf.at[q, peers], recv_sem.at[0, q])
        fbuf[q] = lead_apply(rbuf[q].reshape(GR, LANES), lhi, llo)
        send_to_owners(lambda to: fbuf.at[q, to], gbuf.at[q, own], 1, q)
        gbuf[q, pl.ds(own, 1)] = fbuf[q, pl.ds(own, 1)]

    def add_step(q):
        all_bytes(gbuf.at[q, peers], recv_sem.at[1, q])
        value = gbuf[q].reshape(GR, LANES)
        turned = [value] + [pltpu.roll(value, GROUP * k, 1) for k in (1, 2, 3)]
        for j in range(4):
            spread = turned[(3 - j) % 4]
            for k in range(3):
                spread = jnp.where(lane_group == k, turned[(k - j) % 4], spread)
            high, low = split(jnp.where(lane_group == quarter[q, j], spread, 0.0))
            rhs[j * GR : (j + 1) * GR, 0:LANES] = high
            rhs[j * GR : (j + 1) * GR, LANES:] = low
        if q == 0:
            acc[...] = dot(hot[q], rhs[...])
        else:
            acc[...] += dot(hot[q], rhs[...])

    ahead = NQ // 2
    for q in range(ahead):
        lead_step(q)
    all_bytes(idmine.at[peers], id_recv.at[1])
    unpacked = [None] * AH
    for part in range(AH):
        packed_ids = idmine[...] if AH == 1 else idmine[:, part : part + 1]
        packed_ids = packed_ids.reshape(GR // PACK, LANES)
        wide = jnp.broadcast_to(packed_ids[:, None, :], (GR // PACK, PACK, LANES))
        mine = (iota((GR, LANES), 1) // BN) == (iota((GR, LANES), 0) & (PACK - 1))
        wide = jnp.where(mine, wide.reshape(GR, LANES), 0.0)
        for step in (BN, 2 * BN, 4 * BN):
            wide = wide + pltpu.roll(wide, step, 1)
        unpacked[part] = wide
    ids_in = unpacked[0]
    if AH == 2:
        ids_in = jnp.where((iota((1, LANES), 1) // BN) == 0, unpacked[0], unpacked[1])
    idcol[...] = ids_in.astype(jnp.int32)
    idrow[...] = jnp.transpose(ids_in).astype(jnp.int32)
    for q in range(ahead, NQ):
        build_hot(q - ahead)
        lead_step(q)
    for q in range(NQ):
        if q + NQ - ahead < NQ:
            build_hot(q + NQ - ahead)
        add_step(q)

    packed = acc[:, :LANES] + acc[:, LANES:]
    ZR = QI // ZN
    table[...] = packed.reshape(ZN, ZR, LANES)

    def send_z(k, carry):
        to = lax.rem(zz + k, ZN)
        pltpu.make_async_remote_copy(
            table.at[to],
            zrecv.at[zz],
            z_send.at[0],
            z_recv.at[0],
            device_id=(z_grid(to), s),
            device_id_type=MESH,
        ).start()
        return carry

    lax.fori_loop(1, ZN, send_z, 0)
    zrecv[pl.ds(zz, 1)] = table[pl.ds(zz, 1)]
    zpeers = pl.ds(0, ZN - 1)
    all_bytes(zrecv.at[zpeers], z_recv.at[0])
    total = zrecv[0]
    for k in range(1, ZN):
        total = total + zrecv[k]
    zsum[...] = total

    def send_sum(k, carry):
        to = lax.rem(zz + k, ZN)
        pltpu.make_async_remote_copy(
            zsum,
            tsum.at[zz],
            z_send.at[1],
            z_recv.at[1],
            device_id=(z_grid(to), s),
            device_id_type=MESH,
        ).start()
        return carry

    lax.fori_loop(1, ZN, send_sum, 0)
    tsum[pl.ds(zz, 1)] = total[None]
    def build_lead_back(i, carry):
        row, col = lead_row_col(i)
        dlead[pl.ds(i * RB, RB), :] = backward_entry(row, col).astype(bf16)
        return carry

    lax.fori_loop(0, AH * A // RB, build_lead_back, 0)

    BC = 4
    for c in range(BN // BC):
        row, col = iota((ROWS, BC * AL), 0), iota((ROWS, BC * AL), 1)
        entry = backward_entry(row & (BN - 1), col // AL + c * BC)
        entry = jnp.where(row // BN == (col & (AL - 1)), entry, 0.0)
        dsecond[c] = entry.astype(bf16)
    first = backward_entry(prow // n3, pcol // n3)
    if n3 > 1:
        first = first * backward_entry(prow & (n3 - 1), pcol & (n3 - 1))
    pxs[...] = first
    last_back = backward_entry(qrow // n5, qcol // n5) * backward_entry(
        qrow & (n5 - 1), qcol & (n5 - 1)
    )

    def build_tail_back(i, carry):
        dtail[pl.ds(i * QN, QN), :] = (pxs[pl.ds(i, 1), :] * last_back).astype(bf16)
        return carry

    lax.fori_loop(0, PN, build_tail_back, 0)
    all_bytes(tsum.at[zpeers], z_recv.at[1])
    packed = tsum[...].reshape(QI, LANES)
    high, low = split(packed)
    tsplit[:, 0:LANES] = high
    tsplit[:, LANES:] = low
    even32 = (iota((1, LANES), 1) & 32) == 0

    for q in range(NQ):
        rows_q = dot(hot_t[q], tsplit[...])
        found = []
        for j in range(4):
            row = rows_q[j * GR : (j + 1) * GR]
            row = jnp.where(lane_group == quarter[q, j], row[:, :LANES] + row[:, LANES:], 0.0)
            found.append(row + pltpu.roll(row, 64, 1))
        first = jnp.where(low64, found[0], found[2])
        last = jnp.where(low64, found[1], found[3])
        answer = jnp.where(
            even32, first + pltpu.roll(first, 96, 1), last + pltpu.roll(last, 32, 1)
        )
        abuf[q] = answer.reshape(S, RA, LANES)
        send_to_owners(lambda to: abuf.at[q, to], bbuf.at[q, own], 2, q)
        bbuf[q, pl.ds(own, 1)] = abuf[q, pl.ds(own, 1)]

    for q in range(NQ):
        all_bytes(bbuf.at[q, peers], recv_sem.at[2, q])
        obuf[q] = lead_apply(bbuf[q].reshape(GR, LANES), dlead, None)
        send_to_shards(lambda to: obuf.at[q, to], ubuf.at[q, s], 3, q)
        ubuf[q, pl.ds(s, 1)] = obuf[q, pl.ds(s, 1)]

    CR = ROWS // (BN // 4)
    for q in range(NQ):
        all_bytes(ubuf.at[q, peers], recv_sem.at[3, q])
        for p in range(PG):
            for j, tile in enumerate(swap_groups([ubuf[q, 4 * p + i] for i in range(4)])):
                vbuf[pl.ds(group_row(q, j), RA), pl.ds(p * LANES, LANES)] = tile

        if (q + 1) % AH == 0:
            at = q // AH * CR
            vh, vl = split(vbuf[at : at + CR, :])
            both = dot_t(jnp.concatenate([vh, vl], axis=0), dtail[...])
            yh, yl = split(both[:CR] + both[CR:])
            back = dsecond[q // AH]
            part = dot(back, yh) + dot(back, yl)
            if at == 0:
                out_ref[...] = part
            else:
                out_ref[...] += part
    all_bytes(idall.at[peers], id_send.at[0])
    all_bytes(idall.at[peers], id_send.at[1])
    all_bytes(table.at[zpeers], z_send.at[0])
    all_bytes(tsum.at[zpeers], z_send.at[1])
    for phase in range(4):
        for q in range(NQ):
            all_bytes(wbuf.at[q, peers], send_sem.at[phase, q])


class Config:
    pass


def run_step(cfg, x, coef, shifts, fracs, ids):
    S, ZN, AL, BN, NQ = cfg.shards, cfg.zs, cfg.rows, cfg.second, cfg.chunks
    A, TAIL, NG = cfg.lead, cfg.tail, cfg.ids
    AH, ROWS, QI = PARTS, AL * BN, NG // 4
    RA = AL // AH
    GR = S * RA
    n2, n3, n4, n5 = cfg.tail_dims
    vmem = pl.BlockSpec(memory_space=pltpu.VMEM)
    hbm = pl.BlockSpec(memory_space=pl.ANY)
    V, D = pltpu.VMEM, pltpu.SemaphoreType.DMA
    slabs = V((NQ, S, RA, LANES), f32)
    return pl.pallas_call(
        functools.partial(step_kernel, cfg),
        out_shape=jax.ShapeDtypeStruct((ROWS, TAIL), f32),
        in_specs=[hbm] * 5,
        out_specs=vmem,
        scratch_shapes=[
            pltpu.SMEM(coef.shape, coef.dtype),
            pltpu.SMEM(shifts.shape, shifts.dtype),
            pltpu.SMEM(fracs.shape, fracs.dtype),
            V(ids.shape, ids.dtype),
            V((ROWS, TAIL), f32),
            V((AH * A, GR), bf16),
            V((BN // 4, ROWS, 4 * AL), bf16),
            V((TAIL, TAIL), bf16),
            V((ROWS, ROWS), bf16),
            V((ROWS, ROWS), bf16),
            V((n2 * n3, TAIL), f32),
            V((TAIL, TAIL), bf16),
            V((TAIL, TAIL), bf16),
            V((AH * A, GR), bf16),
            V((AH * A, GR), bf16),
            V((ROWS, TAIL), f32),
            slabs,
            slabs,
            slabs,
            slabs,
            V((AL, LANES), f32),
            V((AL // PACK, LANES), f32),
            V((S, AL // PACK, LANES), f32),
            V((S, AL // PACK, LANES), f32),
            V((GR, LANES), jnp.int32),
            V((LANES, GR), jnp.int32),
            V((NQ, 4, GR, LANES), jnp.int32),
            V((NQ, QI, 4 * GR), bf16),
            V((NQ, 4 * GR, QI), bf16),
            V((4 * GR, 2 * LANES), bf16),
            V((QI, 2 * LANES), f32),
            V((ZN, QI // ZN, LANES), f32),
            V((ZN, QI // ZN, LANES), f32),
            V((QI // ZN, LANES), f32),
            V((ZN, QI // ZN, LANES), f32),
            V((QI, 2 * LANES), bf16),
            slabs,
            slabs,
            slabs,
            slabs,
            D((5,)),
            D((2,)),
            D((2,)),
            D((4, NQ)),
            D((4, NQ)),
            D((2,)),
            D((2,)),
        ],
        compiler_params=pltpu.CompilerParams(
            collective_id=0, has_side_effects=True, vmem_limit_bytes=56 * 1024 * 1024
        ),
    )(coef, shifts, fracs, x, ids)


def build(mesh, tail_dims, id_count):
    def body(density, coefficients, offsets, fractions, subspace_ids):
        _, rows, second, tail = density.shape
        cfg = Config()
        cfg.shards = mesh.shape["shard"]
        cfg.zs = mesh.shape["grid"] // cfg.shards
        cfg.rows, cfg.second, cfg.tail = rows, second, tail
        cfg.lead = rows * cfg.shards
        cfg.chunks = second * GROUP // LANES * PARTS
        cfg.tail_dims, cfg.ids = tail_dims, id_count
        out = run_step(
            cfg,
            density.reshape(rows * second, tail),
            coefficients,
            offsets,
            fractions,
            subspace_ids[0],
        )
        return out.reshape(density.shape)

    return jax.shard_map(
        body,
        mesh=mesh,
        in_specs=(
            P("grid", "shard", None, None),
            P("grid"),
            P("grid", None),
            P("grid", None),
            P("grid", "shard", None),
        ),
        out_specs=P("grid", "shard", None, None),
        check_vma=False,
    )


def solution(mesh):
    return build(mesh, TAIL_DIMS, IDS)
```

```python
import functools

import jax
import jax.numpy as jnp
from jax import lax
from jax.experimental import pallas as pl
from jax.experimental.pallas import tpu as pltpu
from jax.sharding import PartitionSpec as P

MESH = pl.DeviceIdType.MESH
CORES = 2
HALVES = 2
GROUP = 16
LANES = 128
GN = LANES // GROUP
TAIL_DIMS = (8, 4, 4, 4)
IDS = 1024
PACK = 8


f32 = jnp.float32
bf16 = jnp.bfloat16


def iota(shape, dim):
    return lax.broadcasted_iota(jnp.int32, shape, dim)


def split(value):
    high = value.astype(bf16)
    return high, (value - high.astype(f32)).astype(bf16)


def dot(left, right):
    return jnp.dot(left, right, preferred_element_type=f32)


def dot_t(left, right):
    return lax.dot_general(left, right, (((1,), (1,)), ((), ())), preferred_element_type=f32)


def stencil_weights(fraction):
    r = 1.0 - fraction
    sixth = 1.0 / 6.0
    return (
        -r * (r - 1.0) * (r - 2.0) * sixth,
        (r + 1.0) * (r - 1.0) * (r - 2.0) * 0.5,
        -(r + 1.0) * r * (r - 2.0) * 0.5,
        (r + 1.0) * r * (r - 1.0) * sixth,
    )


def sweep(row, col, length, shift, weights):
    step = (col - row + (shift + 2)) & (length - 1)
    out = jnp.where(step == 3, weights[3], 0.0)
    for k in range(3):
        out = jnp.where(step == k, weights[k], out)
    return out


def forward_entry(row, col, length, shift, weights):
    low = row & (-row)
    here = sweep(row, col, length, shift, weights)
    sides = sweep(row - low, col, length, shift, weights) + sweep(
        row + low, col, length, shift, weights
    )
    return jnp.where(row == 0, here, here - 0.5 * sides)


def backward_entry(row, col):
    width = (col & (-col)).astype(f32)
    away = jnp.abs(row - col).astype(f32)
    hat = jnp.maximum(width - away, 0.0) / jnp.where(col == 0, 1.0, width)
    return jnp.where(col == 0, 1.0, hat)


def swap_groups(tiles):
    lane = iota(tiles[0].shape, 1)
    dist = GN // 2
    while dist:
        width = dist * GROUP
        low = (lane & width) == 0
        done = list(tiles)
        for a in range(GN):
            if a & dist == 0:
                b = a + dist
                done[a] = jnp.where(low, tiles[a], pltpu.roll(tiles[b], width, 1))
                done[b] = jnp.where(low, pltpu.roll(tiles[a], LANES - width, 1), tiles[b])
        tiles = done
        dist //= 2
    return tiles


def sum_groups(tiles):
    lane = iota(tiles[0].shape, 1)
    dist = GN // 2
    while dist:
        width = dist * GROUP
        low = (lane & width) == 0
        tiles = [
            jnp.where(
                low,
                tiles[a] + pltpu.roll(tiles[a], LANES - width, 1),
                tiles[a + dist] + pltpu.roll(tiles[a + dist], width, 1),
            )
            for a in range(dist)
        ]
        dist //= 2
    return tiles[0]


def step_kernel(
    cfg,
    coef_hbm,
    shifts_hbm,
    fracs_hbm,
    x_hbm,
    ids_hbm,
    out_ref,
    coef,
    shifts,
    fracs,
    ids_ref,
    xbuf,
    dlead,
    dsecond,
    dtail,
    chi,
    clo,
    pxs,
    thi,
    tlo,
    lhi,
    llo,
    vbuf,
    wbuf,
    rbuf,
    fbuf,
    gbuf,
    idwide,
    idown,
    idall,
    idmine,
    idcol,
    idrow,
    quarter,
    hot,
    hot_t,
    rhs,
    acc,
    table,
    zrecv,
    zsum,
    tsum,
    tsplit,
    abuf,
    bbuf,
    obuf,
    ubuf,
    x_sem,
    id_send,
    id_recv,
    send_sem,
    recv_sem,
    z_send,
    z_recv,
):
    S, ZN, AL, BN, NQ = cfg.shards, cfg.zs, cfg.rows, cfg.second, cfg.chunks
    A, TAIL = cfg.lead, cfg.tail
    ROWS = AL * BN
    NG = cfg.ids
    BH, QI = BN // GN, NG // GN
    GR = S * AL
    g = lax.axis_index("grid")
    s = lax.axis_index("shard")
    core = lax.rem(g, CORES)
    zz = lax.rem(g // CORES, ZN)
    xx = g // (CORES * ZN)
    own = xx * CORES + core

    def owner_grid(o):
        return ((o // CORES) * ZN + zz) * CORES + lax.rem(o, CORES)

    def z_grid(z):
        return (xx * ZN + z) * CORES + core

    copies = [
        pltpu.make_async_copy(src, dst, x_sem.at[k])
        for k, (src, dst) in enumerate(
            [
                (ids_hbm, ids_ref),
                (shifts_hbm, shifts),
                (fracs_hbm, fracs),
                (x_hbm, xbuf),
                (coef_hbm, coef),
            ]
        )
    ]
    for copy in copies:
        copy.start()
    barrier = pltpu.get_barrier_semaphore()

    def far_first(me, send):
        ring = S // 2
        u, v = me // 2, lax.rem(me, 2)

        def body(i, carry):
            sign = 1 - 2 * lax.rem(i, 2)
            step = ring // 2 + sign * ((i + 1) // 2)
            to = lax.rem(u + step + ring, ring) * 2
            send(to + 1 - v)
            send(to + v)
            return carry

        lax.fori_loop(0, ring - 1, body, 0)
        send(u * 2 + 1 - v)

    def greet(grid, shard):
        pl.semaphore_signal(barrier, inc=1, device_id=(grid, shard), device_id_type=MESH)

    far_first(s, lambda to: greet(g, to))
    far_first(own, lambda to: greet(owner_grid(to), s))

    def greet_z(k, carry):
        greet(z_grid(lax.rem(zz + k, ZN)), s)
        return carry

    lax.fori_loop(1, ZN, greet_z, 0)
    copies[0].wait()
    copies[1].wait()
    copies[2].wait()
    weights = [stencil_weights(fracs[0, d]) for d in range(6)]
    shift = [shifts[0, d] for d in range(6)]

    idwide[...] = jnp.zeros_like(idwide)
    idwide[:, 0:BN] = ids_ref[...].astype(f32)
    wide = idwide[...]
    for step in (BN, 2 * BN, 4 * BN):
        wide = wide + pltpu.roll(wide, step, 1)
    mine = (iota((AL, LANES), 1) // BN) == (iota((AL, LANES), 0) & (PACK - 1))
    wide = jnp.where(mine, wide, 0.0)
    for k in range(AL // PACK):
        idown[k : k + 1, :] = jnp.sum(
            wide[k * PACK : (k + 1) * PACK], axis=0, keepdims=True
        )

    RB = 32
    cells = forward_entry(
        iota((BN, ROWS), 0), iota((BN, ROWS), 1) & (BN - 1), BN, shift[1], weights[1]
    )
    own_row = iota((AL, ROWS), 0) == iota((AL, ROWS), 1) // BN
    for b in range(BN):
        high, low = split(jnp.where(own_row, cells[b : b + 1], 0.0))
        chi[b * AL : (b + 1) * AL, :] = high
        clo[b * AL : (b + 1) * AL, :] = low

    n2, n3, n4, n5 = cfg.tail_dims
    PN, QN = n2 * n3, n4 * n5
    prow, pcol = iota((PN, TAIL), 0), iota((PN, TAIL), 1) // QN
    first = forward_entry(prow // n3, pcol // n3, n2, shift[2], weights[2])
    if n3 > 1:
        first = first * forward_entry(
            prow & (n3 - 1), pcol & (n3 - 1), n3, shift[3], weights[3]
        )
    pxs[...] = first
    qrow, qcol = iota((QN, TAIL), 0), iota((QN, TAIL), 1) & (QN - 1)
    last = forward_entry(qrow // n5, qcol // n5, n4, shift[4], weights[4]) * forward_entry(
        qrow & (n5 - 1), qcol & (n5 - 1), n5, shift[5], weights[5]
    )

    def build_tail(i, carry):
        high, low = split(pxs[pl.ds(i, 1), :] * last)
        at = (lax.rem(i, HALVES) * (PN // HALVES) + i // HALVES) * QN
        thi[pl.ds(at, QN), :] = high
        tlo[pl.ds(at, QN), :] = low
        return carry

    lax.fori_loop(0, PN, build_tail, 0)

    copies[3].wait()
    copies[4].wait()
    xh, xl = split(xbuf[...])
    u = dot(chi[...], xh) + dot(chi[...], xl) + dot(clo[...], xh)
    uh, ul = split(u)
    vbuf[...] = dot_t(uh, thi[...]) + dot_t(uh, tlo[...]) + dot_t(ul, thi[...])

    pl.semaphore_wait(barrier, 2 * (S - 1) + (ZN - 1))

    def to_shard(src, dst, send_at, recv_at):
        def send(to):
            pltpu.make_async_remote_copy(
                src(to), dst, send_at, recv_at, device_id=(g, to), device_id_type=MESH
            ).start()

        far_first(s, send)

    def to_owner(src, dst, send_at, recv_at):
        def send(to):
            pltpu.make_async_remote_copy(
                src(to),
                dst,
                send_at,
                recv_at,
                device_id=(owner_grid(to), s),
                device_id_type=MESH,
            ).start()

        far_first(own, send)

    to_shard(lambda to: idown, idall.at[s], id_send.at[0], id_recv.at[0])

    def send_to_shards(src, dst, phase, q):
        to_shard(src, dst, send_sem.at[phase, q], recv_sem.at[phase, q])

    def send_to_owners(src, dst, phase, q):
        to_owner(src, dst, send_sem.at[phase, q], recv_sem.at[phase, q])

    def all_bytes(ref, sem):
        pltpu.make_async_copy(ref, ref, sem).wait()

    peers = pl.ds(0, S - 1)

    HALF = TAIL // HALVES

    def group_row(q, j):
        return (q % BH * GN + j) * AL

    def group_lanes(q, p):
        return pl.ds(q // BH * HALF + p * LANES, LANES)

    for q in range(NQ):
        for p in range(HALF // LANES):
            tiles = [vbuf[pl.ds(group_row(q, j), AL), group_lanes(q, p)] for j in range(GN)]
            for i, tile in enumerate(swap_groups(tiles)):
                wbuf[q, GN * p + i] = tile
        send_to_shards(lambda to: wbuf.at[q, to], rbuf.at[q, s], 0, q)
        rbuf[q, pl.ds(s, 1)] = wbuf[q, pl.ds(s, 1)]

    scale = coef[0].astype(f32)
    scaled = [w * scale for w in weights[0]]

    def lead_row_col(i):
        return iota((RB, A), 0) + i * RB, iota((RB, A), 1)

    def build_lead(i, carry):
        row, col = lead_row_col(i)
        high, low = split(forward_entry(row, col, A, shift[0], scaled))
        lhi[pl.ds(i * RB, RB), :] = high
        llo[pl.ds(i * RB, RB), :] = low
        return carry

    lax.fori_loop(0, A // RB, build_lead, 0)

    def lead_apply(value, high, low):
        vh, vl = split(value)
        both = dot(high[...], jnp.concatenate([vh, vl], axis=1))
        out = both[:, :LANES] + both[:, LANES:]
        if low is not None:
            out = out + dot(low[...], vh)
        return out.reshape(S, AL, LANES)

    idall[pl.ds(s, 1)] = idown[...][None]
    all_bytes(idall.at[peers], id_recv.at[0])

    to_owner(lambda to: idall.at[to], idmine.at[own], id_send.at[1], id_recv.at[1])
    idmine[pl.ds(own, 1)] = idall[pl.ds(own, 1)]

    def build_hot(h):
        for j in range(GN):
            at = h * GN + j
            ids_here = idrow[at : at + 1, :] & (QI - 1)
            hot[h, :, j * GR : (j + 1) * GR] = jnp.where(
                iota((QI, GR), 0) == ids_here, 1.0, 0.0
            ).astype(bf16)
            column = idcol[:, at : at + 1]
            quarter[h, j] = jnp.broadcast_to(column // QI, (GR, LANES))
            hot_t[h, j * GR : (j + 1) * GR, :] = jnp.where(
                iota((GR, QI), 1) == (column & (QI - 1)), 1.0, 0.0
            ).astype(bf16)

    lane_group = iota((1, LANES), 1) // GROUP

    def lead_step(q):
        all_bytes(rbuf.at[q, peers], recv_sem.at[0, q])
        fbuf[q] = lead_apply(rbuf[q].reshape(GR, LANES), lhi, llo)
        send_to_owners(lambda to: fbuf.at[q, to], gbuf.at[q, own], 1, q)
        gbuf[q, pl.ds(own, 1)] = fbuf[q, pl.ds(own, 1)]

    def add_step(q):
        all_bytes(gbuf.at[q, peers], recv_sem.at[1, q])
        half, h = q // BH, q % BH
        value = gbuf[q].reshape(GR, LANES)
        for at in range(0, GR, RB):
            here = value[at : at + RB]
            turned = [here] + [pltpu.roll(here, GROUP * k, 1) for k in range(1, GN)]
            for j in range(GN):
                spread = turned[(GN - 1 - j) % GN]
                for k in range(GN - 1):
                    spread = jnp.where(lane_group == k, turned[(k - j) % GN], spread)
                mine = lane_group == quarter[h, j, at : at + RB]
                high, low = split(jnp.where(mine, spread, 0.0))
                rhs[j * GR + at : j * GR + at + RB, 0:LANES] = high
                rhs[j * GR + at : j * GR + at + RB, LANES:] = low
        if h == 0:
            acc[half] = dot(hot[h], rhs[...])
        else:
            acc[half] += dot(hot[h], rhs[...])

    ahead = NQ // 2
    for q in range(ahead):
        lead_step(q)
    all_bytes(idmine.at[peers], id_recv.at[1])
    packed_ids = idmine[...].reshape(GR // PACK, LANES)
    ids_in = jnp.broadcast_to(packed_ids[:, None, :], (GR // PACK, PACK, LANES))
    mine = (iota((GR, LANES), 1) // BN) == (iota((GR, LANES), 0) & (PACK - 1))
    ids_in = jnp.where(mine, ids_in.reshape(GR, LANES), 0.0)
    for step in (BN, 2 * BN, 4 * BN):
        ids_in = ids_in + pltpu.roll(ids_in, step, 1)
    idcol[...] = ids_in.astype(jnp.int32)
    idrow[...] = jnp.transpose(ids_in).astype(jnp.int32)
    for q in range(ahead, NQ):
        build_hot(q - ahead)
        lead_step(q)

    ZR = QI // ZN
    zpeers = pl.ds(0, ZN - 1)

    def to_z(src, dst, at):
        def send(k, carry):
            to = lax.rem(zz + ZN - k, ZN)
            pltpu.make_async_remote_copy(
                src(to),
                dst,
                z_send.at[at],
                z_recv.at[at],
                device_id=(z_grid(to), s),
                device_id_type=MESH,
            ).start()
            return carry

        lax.fori_loop(1, ZN, send, 0)

    def sum_start(half):
        packed = acc[half, :, :LANES] + acc[half, :, LANES:]
        table[half] = packed.reshape(ZN, ZR, LANES)
        to_z(lambda to: table.at[half, to], zrecv.at[half, zz], 2 * half)
        zrecv[half, pl.ds(zz, 1)] = table[half, pl.ds(zz, 1)]

    def sum_middle(half):
        all_bytes(zrecv.at[half, zpeers], z_recv.at[2 * half])
        total = zrecv[half, 0]
        for k in range(1, ZN):
            total = total + zrecv[half, k]
        zsum[half] = total
        to_z(lambda to: zsum.at[half], tsum.at[half, zz], 2 * half + 1)
        tsum[half, pl.ds(zz, 1)] = total[None]

    def sum_end(half):
        all_bytes(tsum.at[half, zpeers], z_recv.at[2 * half + 1])
        high, low = split(tsum[half].reshape(QI, LANES))
        tsplit[half, :, 0:LANES] = high
        tsplit[half, :, LANES:] = low

    def answer_step(q):
        half, h = q // BH, q % BH
        rows_q = dot(hot_t[h], tsplit[half])
        found = []
        for j in range(GN):
            row = rows_q[j * GR : (j + 1) * GR]
            found.append(
                jnp.where(lane_group == quarter[h, j], row[:, :LANES] + row[:, LANES:], 0.0)
            )
        abuf[q] = sum_groups(found).reshape(S, AL, LANES)
        send_to_owners(lambda to: abuf.at[q, to], bbuf.at[q, own], 2, q)
        bbuf[q, pl.ds(own, 1)] = abuf[q, pl.ds(own, 1)]

    add_step(0)
    add_step(1)
    sum_start(0)
    add_step(2)
    sum_middle(0)
    add_step(3)
    sum_start(1)
    sum_end(0)
    answer_step(0)
    sum_middle(1)
    answer_step(1)
    def build_lead_back(i, carry):
        row, col = lead_row_col(i)
        dlead[pl.ds(i * RB, RB), :] = backward_entry(row, col).astype(bf16)
        return carry

    lax.fori_loop(0, A // RB, build_lead_back, 0)

    BC = GN
    for c in range(BN // BC):
        row, col = iota((ROWS, BC * AL), 0), iota((ROWS, BC * AL), 1)
        entry = backward_entry(row & (BN - 1), col // AL + c * BC)
        entry = jnp.where(row // BN == (col & (AL - 1)), entry, 0.0)
        dsecond[c] = entry.astype(bf16)
    spot = iota((PN, TAIL), 1)
    pback = spot % HALF // QN * HALVES + spot // HALF
    first = backward_entry(prow // n3, pback // n3)
    if n3 > 1:
        first = first * backward_entry(prow & (n3 - 1), pback & (n3 - 1))
    pxs[...] = first
    last_back = backward_entry(qrow // n5, qcol // n5) * backward_entry(
        qrow & (n5 - 1), qcol & (n5 - 1)
    )

    def build_tail_back(i, carry):
        dtail[pl.ds(i * QN, QN), :] = (pxs[pl.ds(i, 1), :] * last_back).astype(bf16)
        return carry

    lax.fori_loop(0, PN, build_tail_back, 0)
    sum_end(1)
    answer_step(2)
    answer_step(3)

    for q in range(NQ):
        all_bytes(bbuf.at[q, peers], recv_sem.at[2, q])
        obuf[q] = lead_apply(bbuf[q].reshape(GR, LANES), dlead, None)
        send_to_shards(lambda to: obuf.at[q, to], ubuf.at[q, s], 3, q)
        ubuf[q, pl.ds(s, 1)] = obuf[q, pl.ds(s, 1)]

    CR = GN * AL
    for q in range(NQ):
        all_bytes(ubuf.at[q, peers], recv_sem.at[3, q])
        for p in range(HALF // LANES):
            tiles = [ubuf[q, GN * p + i] for i in range(GN)]
            for j, tile in enumerate(swap_groups(tiles)):
                vbuf[pl.ds(group_row(q, j), AL), group_lanes(q, p)] = tile
        lanes = slice(q // BH * HALF, (q // BH + 1) * HALF)
        vh, vl = split(vbuf[q % BH * CR : (q % BH + 1) * CR, lanes])
        both = dot_t(jnp.concatenate([vh, vl], axis=0), dtail[:, lanes])
        yh, yl = split(both[:CR] + both[CR:])
        part = dot(dsecond[q % BH], yh) + dot(dsecond[q % BH], yl)
        if q == 0:
            out_ref[...] = part
        else:
            out_ref[...] += part
    all_bytes(idall.at[peers], id_send.at[0])
    all_bytes(idall.at[peers], id_send.at[1])
    for half in range(HALVES):
        all_bytes(table.at[half, zpeers], z_send.at[2 * half])
        all_bytes(tsum.at[half, zpeers], z_send.at[2 * half + 1])
    for phase in range(4):
        for q in range(NQ):
            all_bytes(wbuf.at[q, peers], send_sem.at[phase, q])


class Config:
    pass


def run_step(cfg, x, coef, shifts, fracs, ids):
    S, ZN, AL, BN, NQ = cfg.shards, cfg.zs, cfg.rows, cfg.second, cfg.chunks
    A, TAIL, NG = cfg.lead, cfg.tail, cfg.ids
    ROWS, QI, BH = AL * BN, NG // GN, BN // GN
    GR = S * AL
    n2, n3, n4, n5 = cfg.tail_dims
    vmem = pl.BlockSpec(memory_space=pltpu.VMEM)
    hbm = pl.BlockSpec(memory_space=pl.ANY)
    V, D = pltpu.VMEM, pltpu.SemaphoreType.DMA
    slabs = V((NQ, S, AL, LANES), f32)
    return pl.pallas_call(
        functools.partial(step_kernel, cfg),
        out_shape=pltpu.VMEM((ROWS, TAIL), f32),
        in_specs=[hbm] * 5,
        out_specs=vmem,
        scratch_shapes=[
            pltpu.SMEM(coef.shape, coef.dtype),
            pltpu.SMEM(shifts.shape, shifts.dtype),
            pltpu.SMEM(fracs.shape, fracs.dtype),
            V(ids.shape, ids.dtype),
            V((ROWS, TAIL), f32),
            V((A, A), bf16),
            V((BH, ROWS, GN * AL), bf16),
            V((TAIL, TAIL), bf16),
            V((ROWS, ROWS), bf16),
            V((ROWS, ROWS), bf16),
            V((n2 * n3, TAIL), f32),
            V((TAIL, TAIL), bf16),
            V((TAIL, TAIL), bf16),
            V((A, A), bf16),
            V((A, A), bf16),
            V((ROWS, TAIL), f32),
            slabs,
            slabs,
            slabs,
            slabs,
            V((AL, LANES), f32),
            V((AL // PACK, LANES), f32),
            V((S, AL // PACK, LANES), f32),
            V((S, AL // PACK, LANES), f32),
            V((GR, LANES), jnp.int32),
            V((LANES, GR), jnp.int32),
            V((BH, GN, GR, LANES), jnp.int32),
            V((BH, QI, GN * GR), bf16),
            V((BH, GN * GR, QI), bf16),
            V((GN * GR, 2 * LANES), bf16),
            V((HALVES, QI, 2 * LANES), f32),
            V((HALVES, ZN, QI // ZN, LANES), f32),
            V((HALVES, ZN, QI // ZN, LANES), f32),
            V((HALVES, QI // ZN, LANES), f32),
            V((HALVES, ZN, QI // ZN, LANES), f32),
            V((HALVES, QI, 2 * LANES), bf16),
            slabs,
            slabs,
            slabs,
            slabs,
            D((5,)),
            D((2,)),
            D((2,)),
            D((4, NQ)),
            D((4, NQ)),
            D((2 * HALVES,)),
            D((2 * HALVES,)),
        ],
        compiler_params=pltpu.CompilerParams(
            collective_id=0, has_side_effects=True, vmem_limit_bytes=56 * 1024 * 1024
        ),
    )(coef, shifts, fracs, x, ids)


def build(mesh, tail_dims, id_count):
    def body(density, coefficients, offsets, fractions, subspace_ids):
        _, rows, second, tail = density.shape
        cfg = Config()
        cfg.shards = mesh.shape["shard"]
        cfg.zs = mesh.shape["grid"] // cfg.shards
        cfg.rows, cfg.second, cfg.tail = rows, second, tail
        cfg.lead = rows * cfg.shards
        cfg.chunks = HALVES * second * GROUP // LANES
        cfg.tail_dims, cfg.ids = tail_dims, id_count
        out = run_step(
            cfg,
            density.reshape(rows * second, tail),
            coefficients,
            offsets,
            fractions,
            subspace_ids[0],
        )
        return out.reshape(density.shape)

    return jax.shard_map(
        body,
        mesh=mesh,
        in_specs=(
            P("grid", "shard", None, None),
            P("grid"),
            P("grid", None),
            P("grid", None),
            P("grid", "shard", None),
        ),
        out_specs=P("grid", "shard", None, None),
        check_vma=False,
    )


def solution(mesh):
    return build(mesh, TAIL_DIMS, IDS)
```
